32 devices in a mesh: groups: 2 (over x), bay: 16 (over z, y, core).
Axes of the slice: x: 2, y: 2, z: 4, core: 2. Of those that a mesh axis runs over, the one named last changes fastest.
Arguments:
- traces: bfloat16 [16, 512, 2048], P('bay', 'groups'), parts along dimension 1, may hold values from -6 to 6
- operator: bfloat16 [16, 2048, 2048], P('bay'), may hold values from -0.09375 to 0.09375
- loads: bfloat16 [16, 16, 2048], P('bay'), may hold values from -6 to 6
- seeds: int32 [512], P('groups'), parts along dimension 0, may hold values from 0 to 99999
- patches: int32 [16, 512], P('bay', 'groups'), parts along dimension 1, may hold values from 0 to 15
- trace_map: int32 [16, 1024], P('bay'), may hold values from 0 to 1023, each once within a row
Outputs:
- final_traces: bfloat16 [16, 512, 2048], P('bay', 'groups'), parts along dimension 1
The draws below stay inside these ranges and needn't reach their ends.
There are 2 independent parts, one for each index of `groups`. The reference program is written for one: setup_inputs(seed, part) draws one part's arguments, and reference() takes and returns one part's arrays. A program takes and returns all parts, laid end to end along the dimension named above; an argument that names none is the same for every part. Nothing has to cross between parts.
Inputs may be any that keep to these rules, and one draw needn't show every extreme that they name: `trace_map`: each row is a permutation of 0 to 1023.
All inputs are finite; a program needn't handle non-finite values.
Results may differ from the reference program's by a relative error of at most 0.0065.
Values may be sent and summed in bfloat16 or wider, within the bound.
No kernel may reach another device: no remote copies, remote signals or barrier semaphores. Data moves between devices by JAX's collectives and lax.ppermute only.
A program may use at most 64 MiB of HBM per device.

```python
import jax
import jax.numpy as jnp
from jax import lax

TRACES = 2048
ONWARD = 1024
LATERAL = 512
CASES = 256
TICKS = 6
STRIPS = 4
PATCHES = 16
N_BAY = 16


def plant(drawn, rng, least, largest):
    dims = drawn.shape
    index_at = [jax.random.randint(jax.random.fold_in(rng, axis), (), 0, dims[axis]) for axis in range(len(dims))]
    drawn = drawn.at[tuple(index_at)].set(least)
    longest = dims.index(max(dims))
    index_at[longest] = (index_at[longest] + 1) % dims[longest]
    return drawn.at[tuple(index_at)].set(largest)


def block_levels(own_key, extent, pieces, least, high):
    level, own = 1.0, jax.random.fold_in(own_key, 6)
    for dim, shards_of in pieces:
        steps = jnp.exp(jax.random.uniform(jax.random.fold_in(own, dim), (shards_of,), jnp.float32, least / len(pieces), high / len(pieces)))
        level = level * jnp.repeat(steps, extent[dim] // shards_of).reshape([-1 if axis == dim else 1 for axis in range(len(extent))])
    return level


def normal_values(stream_key, shape, scale, reach, shards=(), kind=jnp.bfloat16):
    entries = scale * jax.random.normal(stream_key, shape, jnp.float32)
    if shards:
        entries = entries * block_levels(stream_key, shape, shards, -0.22, 0.18)
    return jnp.clip(entries, -reach, reach).astype(kind)


def setup_inputs(seed: int = 0, part: int = 0) -> dict:
    splits = jax.random.split(jax.random.key(seed), 7)
    part_splits = jax.random.split(jax.random.fold_in(splits[6], part), 7)
    traces = normal_values(part_splits[0], (N_BAY, CASES, TRACES), 1.0, 6.0, ((0, 16),))
    operator = normal_values(splits[1], (N_BAY, TRACES, TRACES), (2 * TRACES) ** -0.5, 0.09375, ((0, 16),))
    loads = normal_values(splits[2], (N_BAY, PATCHES, TRACES), 1.0, 6.0, ((0, 16),))
    seeds = plant(jax.random.randint(part_splits[3], (CASES,), 0, 100000), jax.random.fold_in(part_splits[3], 1), 0, 99999).astype(jnp.int32)
    patches = plant(jax.random.randint(part_splits[4], (N_BAY, CASES), 0, PATCHES), jax.random.fold_in(part_splits[4], 1), 0, PATCHES - 1).astype(jnp.int32)
    trace_map = jax.vmap(lambda own: jax.random.permutation(own, ONWARD))(jax.random.split(splits[5], N_BAY)).reshape((N_BAY, ONWARD)).astype(jnp.int32)
    return {"traces": traces, "operator": operator, "loads": loads, "seeds": seeds, "patches": patches, "trace_map": trace_map}


def reference(traces, operator, loads, seeds, patches, trace_map):
    index = jnp.arange(N_BAY, dtype=jnp.int32)
    near_ids = jnp.bitwise_xor(index, 1)
    far_ids = jnp.bitwise_xor(index, 2)
    patch_rows = jax.vmap(lambda table, picks: jnp.take(table, picks, axis=0))(loads, patches).astype(jnp.float32)
    state = traces
    for tick in range(TICKS):
        amplitude = (((seeds * 7 + 13 * tick) % 97) - 48).astype(jnp.float32) / 32.0
        source = amplitude[None, :, None] * patch_rows
        onward = state[:, :, :ONWARD]
        shifted = jnp.concatenate([jnp.zeros((STRIPS, CASES, ONWARD), jnp.bfloat16), onward[:N_BAY - STRIPS]], axis=0)
        mapped = jax.vmap(lambda block, order: jnp.take(block, order, axis=1))(shifted, trace_map)
        near = state[near_ids][:, :, ONWARD:ONWARD + LATERAL]
        far = state[far_ids][:, :, ONWARD + LATERAL:]
        incoming = jnp.concatenate([mapped, near, far], axis=2)
        product = lax.map(lambda pair: jnp.dot(pair[0], pair[1], preferred_element_type=jnp.float32), (incoming, operator))
        state = (product + source).astype(jnp.bfloat16)
    return state
```

```python
import functools

import jax
import jax.numpy as jnp
from jax import lax
from jax.experimental import pallas as pl
from jax.experimental.pallas import tpu as pltpu
from jax.sharding import PartitionSpec as P

TICKS = 6
STRIPS = 4
CHUNKS = 2
COLS = 512
RING = True


VMEM = pl.BlockSpec(memory_space=pltpu.VMEM)


def onward_pairs(count):
    if RING:
        return [(source, (source + STRIPS) % count) for source in range(count)]
    return [(source, source + STRIPS) for source in range(count - STRIPS)]


def exchange(pieces, count):
    onward, near, far = pieces
    got_onward = lax.ppermute(onward, "bay", onward_pairs(count))
    got_near = lax.ppermute(near, "bay", [(i, i ^ 1) for i in range(count)])
    got_far = lax.ppermute(far, "bay", [(i, i ^ 2) for i in range(count)])
    return got_onward, got_near, got_far


def reorder_body(order, weights, out):
    size = order.shape[1]
    step = min(256, size)
    for low in range(0, size, step):
        rows = low + lax.broadcasted_iota(jnp.int32, (step, size), 0)
        select = (order[...] == rows).astype(jnp.bfloat16)
        out[low : low + step, :] = jnp.dot(
            select, weights[:size, :], preferred_element_type=jnp.float32
        ).astype(jnp.bfloat16)


def reorder(order, weights):
    size, width = order.shape[1], weights.shape[1]
    return pl.pallas_call(
        reorder_body,
        out_shape=jax.ShapeDtypeStruct((size, width), jnp.bfloat16),
        in_specs=[VMEM, VMEM],
        out_specs=VMEM,
        name="reorder",
        compiler_params=pltpu.CompilerParams(vmem_limit_bytes=24 << 20),
        cost_estimate=pl.CostEstimate(
            flops=2 * size * size * width, transcendentals=0, bytes_accessed=3 * size * width * 2
        ),
    )(order, weights)


def block(tick, low, high, onward, near, far, upper, weights, amps, patch):
    first = onward.shape[1]
    second = first + near.shape[1]
    total = jnp.dot(near[...], weights[first:second, low:high], preferred_element_type=jnp.float32)
    total += jnp.dot(far[...], weights[second:, low:high], preferred_element_type=jnp.float32)
    total += jnp.dot(onward[...], upper[:, low:high], preferred_element_type=jnp.float32)
    total += amps[:, tick : tick + 1] * patch[:, low:high].astype(jnp.float32)
    return total.astype(jnp.bfloat16)


def step_body(tick, onward, near, far, upper, weights, amps, patch, out_onward, out_near, out_far):
    start = 0
    for out in (out_onward, out_near, out_far):
        for low in range(0, out.shape[1], COLS):
            out[:, low : low + COLS] = block(
                tick, start + low, start + low + COLS, onward, near, far, upper, weights, amps, patch
            )
        start += out.shape[1]


def cost(rows, weights):
    return pl.CostEstimate(
        flops=2 * rows * weights.shape[0] * weights.shape[1],
        transcendentals=0,
        bytes_accessed=weights.size * 2,
    )


def step(tick, got, upper, weights, amps, patch):
    rows = amps.shape[0]
    return pl.pallas_call(
        functools.partial(step_body, tick),
        out_shape=tuple(jax.ShapeDtypeStruct(piece.shape, jnp.bfloat16) for piece in got),
        in_specs=[VMEM] * 7,
        out_specs=(VMEM,) * 3,
        name=f"step{tick}",
        compiler_params=pltpu.CompilerParams(vmem_limit_bytes=16 << 20),
        cost_estimate=cost(rows, weights),
    )(*got, upper, weights, amps, patch)


def last_body(tick, chunk, onward, near, far, upper, weights, amps, patch, *rest):
    out, buffer, sems = rest[-3:]
    rows, width = buffer.shape
    copies = []
    for index, low in enumerate(range(0, width, COLS)):
        buffer[:, low : low + COLS] = block(
            tick, low, low + COLS, onward, near, far, upper, weights, amps, patch
        )
        copies.append(
            pltpu.make_async_copy(
                buffer.at[:, low : low + COLS],
                out.at[0, chunk * rows : (chunk + 1) * rows, low : low + COLS],
                sems.at[index],
            )
        )
        copies[-1].start()
    for copy in copies:
        copy.wait()


def last_step(tick, chunk, chunks, got, upper, weights, amps, patch, previous):
    rows, width = patch.shape
    extra = [] if previous is None else [previous]
    return pl.pallas_call(
        functools.partial(last_body, tick, chunk),
        out_shape=jax.ShapeDtypeStruct((1, rows * chunks, width), jnp.bfloat16),
        in_specs=[VMEM] * 7 + [pl.BlockSpec(memory_space=pl.ANY)] * len(extra),
        out_specs=pl.BlockSpec(memory_space=pl.ANY),
        scratch_shapes=[
            pltpu.VMEM((rows, width), jnp.bfloat16),
            pltpu.SemaphoreType.DMA((pl.cdiv(width, COLS),)),
        ],
        input_output_aliases={7: 0} if extra else {},
        name="last",
        compiler_params=pltpu.CompilerParams(vmem_limit_bytes=16 << 20),
        cost_estimate=cost(rows, weights),
    )(*got, upper, weights, amps, patch, *extra)


def on_device(traces, operator, loads, seeds, patches, trace_map):
    count = lax.axis_size("bay")
    state = traces[0]
    weights = operator[0]
    rows, width = state.shape
    onward = trace_map.shape[1]
    lateral = (width - onward) // 2
    size = rows // CHUNKS

    got = []
    for c in range(CHUNKS):
        part = state[c * size : (c + 1) * size]
        pieces = (part[:, :onward], part[:, onward : onward + lateral], part[:, onward + lateral :])
        got.append(exchange(pieces, count))

    has_previous = lax.axis_index("bay") >= STRIPS
    order = jnp.where(has_previous, trace_map, -1)
    upper = reorder(order, weights)
    table = loads[0]
    one_hot = (patches[0][:, None] == jnp.arange(table.shape[0], dtype=jnp.int32)[None, :]).astype(
        jnp.bfloat16
    )
    patch = jnp.dot(one_hot, table, preferred_element_type=jnp.float32).astype(jnp.bfloat16)
    ticks = jnp.arange(TICKS, dtype=jnp.int32)[None, :]
    amps = ((seeds[:, None] * 7 + 13 * ticks) % 97 - 48).astype(jnp.float32) / 32.0

    out = None
    for tick in range(TICKS):
        for c in range(CHUNKS):
            own = slice(c * size, (c + 1) * size)
            common = (got[c], upper, weights, amps[own], patch[own])
            if tick == TICKS - 1:
                out = last_step(tick, c, CHUNKS, *common, out)
            else:
                got[c] = exchange(step(tick, *common), count)
    return out


def solution(mesh):
    placed = (
        P("bay", "groups", None),
        P("bay", None, None),
        P("bay", None, None),
        P("groups"),
        P("bay", "groups"),
        P("bay", None),
    )
    return jax.shard_map(
        on_device, mesh=mesh, in_specs=placed, out_specs=P("bay", "groups", None), check_vma=False
    )
```

```python
import functools

import jax
import jax.numpy as jnp
from jax import lax
from jax.experimental import pallas as pl
from jax.experimental.pallas import tpu as pltpu
from jax.sharding import PartitionSpec as P


TICKS = 6
STRIPS = 4
CHUNKS = 2
COLS = 512
EARLY = 6
LIMIT = 16 << 20


VMEM = pl.BlockSpec(memory_space=pltpu.VMEM)
HBM = pl.BlockSpec(memory_space=pltpu.HBM)
ANY = pl.BlockSpec(memory_space=pl.ANY)


def exchange(pieces, count, wrap=True):
    onward, near, far = pieces
    stop = count if wrap else count - STRIPS
    got_onward = lax.ppermute(
        onward, "bay", [(i, (i + STRIPS) % count) for i in range(stop)]
    )
    got_near = lax.ppermute(near, "bay", [(i, i ^ 1) for i in range(count)])
    got_far = lax.ppermute(far, "bay", [(i, i ^ 2) for i in range(count)])
    return got_onward, got_near, got_far


def fetch(source, outs, spans, sems):
    copies = []
    for index, (out, (rows, columns)) in enumerate(zip(outs, spans)):
        copies.append(pltpu.make_async_copy(source.at[0, rows, columns], out, sems.at[index]))
        copies[-1].start()
    return copies


def cut_body(spans, source, *rest):
    *outs, sems = rest
    for copy in fetch(source, outs, spans, sems):
        copy.wait()


def load_body(spans, trace_map, source, operator, table, *rest):
    *outs, select, weights, loads, order, sems = rest
    fetch_order = pltpu.make_async_copy(trace_map, order, sems.at[len(spans) + 2])
    fetch_order.start()
    copies = fetch(source, outs, spans, sems)
    for index, (whole, out) in enumerate(((operator, weights), (table, loads))):
        copies.append(pltpu.make_async_copy(whole.at[0], out, sems.at[len(spans) + index]))
        copies[-1].start()
    size = order.shape[1]
    block = min(256, size)
    fetch_order.wait()
    wanted = jnp.where(lax.axis_index("bay") >= STRIPS, order[...], -1)
    for top in range(0, size, block):
        rows = top + lax.broadcasted_iota(jnp.int32, (block, size), 0)
        select[top : top + block, :] = (wanted == rows).astype(jnp.bfloat16)
    for copy in copies:
        copy.wait()


def shape_of(span):
    return jax.ShapeDtypeStruct(tuple(part.stop - part.start for part in span), jnp.bfloat16)


def in_hbm(*arrays):
    return [pltpu.with_memory_space_constraint(array, pltpu.HBM) for array in arrays]


def cut(traces, spans):
    return pl.pallas_call(
        functools.partial(cut_body, spans),
        out_shape=tuple(shape_of(span) for span in spans),
        in_specs=[HBM],
        out_specs=(VMEM,) * len(spans),
        scratch_shapes=[pltpu.SemaphoreType.DMA((len(spans),))],
        name="cut",
        compiler_params=pltpu.CompilerParams(vmem_limit_bytes=LIMIT),
    )(*in_hbm(traces))


def load(order, traces, spans, operator, loads):
    shapes = [shape_of(span) for span in spans]
    shapes.append(jax.ShapeDtypeStruct((order.shape[1],) * 2, jnp.bfloat16))
    shapes.extend(jax.ShapeDtypeStruct(whole.shape[1:], jnp.bfloat16) for whole in (operator, loads))
    return pl.pallas_call(
        functools.partial(load_body, spans),
        out_shape=tuple(shapes),
        in_specs=[HBM] * 4,
        out_specs=(VMEM,) * len(shapes),
        scratch_shapes=[
            pltpu.VMEM(order.shape, order.dtype),
            pltpu.SemaphoreType.DMA((len(spans) + 3,)),
        ],
        name="load",
        compiler_params=pltpu.CompilerParams(vmem_limit_bytes=LIMIT),
    )(*in_hbm(order, traces, operator, loads))


def prepared(tick, chunk, onward, select, seeds, patches, table):
    size = onward.shape[0]
    own = slice(chunk * size, (chunk + 1) * size)
    mapped = jnp.dot(onward[...], select[...], preferred_element_type=jnp.float32).astype(
        jnp.bfloat16
    )
    amplitude = ((seeds[:, own] * 7 + 13 * tick) % 97 - 48).astype(jnp.float32) / 32.0
    rows = lax.broadcasted_iota(jnp.int32, (table.shape[0], size), 0)
    loaded = jnp.where(rows == patches[:, own], amplitude, 0.0).astype(jnp.bfloat16)
    return mapped, loaded


def block(mapped, loaded, near, far, weights, table, low, high):
    first = mapped.shape[1]
    second = first + near.shape[1]
    total = jnp.dot(near[...], weights[first:second, low:high], preferred_element_type=jnp.float32)
    total += jnp.dot(far[...], weights[second:, low:high], preferred_element_type=jnp.float32)
    total += lax.dot_general(
        loaded, table[:, low:high], (((0,), (0,)), ((), ())), preferred_element_type=jnp.float32
    )
    total += jnp.dot(mapped, weights[:first, low:high], preferred_element_type=jnp.float32)
    return total.astype(jnp.bfloat16)


def step_body(tick, chunk, onward, near, far, select, seeds, patches, table, weights, *outs):
    mapped, loaded = prepared(tick, chunk, onward, select, seeds, patches, table)
    start = 0
    for out in outs:
        for low in range(0, out.shape[1], COLS):
            out[:, low : low + COLS] = block(
                mapped, loaded, near, far, weights, table, start + low, start + low + COLS
            )
        start += out.shape[1]


def cost(rows, weights):
    return pl.CostEstimate(
        flops=2 * rows * weights.shape[0] * weights.shape[1],
        transcendentals=0,
        bytes_accessed=weights.size * 2,
    )


def step(tick, chunk, got, common, weights):
    return pl.pallas_call(
        functools.partial(step_body, tick, chunk),
        out_shape=tuple(jax.ShapeDtypeStruct(piece.shape, jnp.bfloat16) for piece in got),
        in_specs=[VMEM] * 8,
        out_specs=(VMEM,) * 3,
        compiler_params=pltpu.CompilerParams(vmem_limit_bytes=LIMIT),
        cost_estimate=cost(got[0].shape[0], weights),
    )(*got, *common, weights)


def last_body(tick, chunk, onward, near, far, select, seeds, patches, table, weights, *rest):
    out, buffer, sems = rest[-3:]
    rows, width = buffer.shape
    mapped, loaded = prepared(tick, chunk, onward, select, seeds, patches, table)
    copies = []
    for index, low in enumerate(range(0, width, COLS)):
        buffer[:, low : low + COLS] = block(
            mapped, loaded, near, far, weights, table, low, low + COLS
        )
        copies.append(
            pltpu.make_async_copy(
                buffer.at[:, low : low + COLS],
                out.at[0, chunk * rows : (chunk + 1) * rows, low : low + COLS],
                sems.at[index],
            )
        )
        copies[-1].start()
    for copy in copies:
        copy.wait()


def last_step(tick, chunk, got, common, weights, previous):
    rows, width = got[0].shape[0], weights.shape[1]
    extra = [] if previous is None else [previous]
    return pl.pallas_call(
        functools.partial(last_body, tick, chunk),
        out_shape=jax.ShapeDtypeStruct((1, rows * CHUNKS, width), jnp.bfloat16),
        in_specs=[VMEM] * 8 + [ANY] * len(extra),
        out_specs=ANY,
        scratch_shapes=[
            pltpu.VMEM((rows, width), jnp.bfloat16),
            pltpu.SemaphoreType.DMA((pl.cdiv(width, COLS),)),
        ],
        input_output_aliases={8: 0} if extra else {},
        name="last",
        compiler_params=pltpu.CompilerParams(vmem_limit_bytes=LIMIT),
        cost_estimate=cost(rows, weights),
    )(*got, *common, weights, *extra)


def on_device(traces, operator, loads, seeds, patches, trace_map):
    count = lax.axis_size("bay")
    _, rows, width = traces.shape
    onward = trace_map.shape[1]
    near = onward + (width - onward) // 2
    size = rows // CHUNKS
    columns = (slice(0, onward), slice(onward, near), slice(near, width))
    spans = [
        [(slice(c * size, (c + 1) * size), piece) for piece in columns] for c in range(CHUNKS)
    ]
    flat = [span for part in spans for span in part]

    pieces = cut(traces, flat[:EARLY])
    *others, select, weights, table = load(trace_map, traces, flat[EARLY:], operator, loads)
    pieces = [*pieces, *others]
    got = []
    for c in range(CHUNKS):
        got.append(exchange(pieces[3 * c : 3 * c + 3], count))

    common = (select, seeds[None], patches, table)
    out = None
    for tick in range(TICKS):
        for c in range(CHUNKS):
            if tick == TICKS - 1:
                out = last_step(tick, c, got[c], common, weights, out)
            else:
                pieces = step(tick, c, got[c], common, weights)
                got[c] = exchange(pieces, count, tick + 2 < TICKS)
    return out


def solution(mesh):
    placed = (
        P("bay", "groups", None),
        P("bay", None, None),
        P("bay", None, None),
        P("groups"),
        P("bay", "groups"),
        P("bay", None),
    )
    return jax.shard_map(
        on_device, mesh=mesh, in_specs=placed, out_specs=P("bay", "groups", None), check_vma=False
    )
```

```python
import functools

import jax
import jax.numpy as jnp
from jax import lax
from jax.experimental import pallas as pl
from jax.experimental.pallas import tpu as pltpu
from jax.sharding import PartitionSpec as P


TICKS = 6
STRIPS = 4
CHUNKS = 2
COLS = 512
EARLY = 6
PARTS = 8
SPARE = 0
LIMIT = 16 << 20


VMEM = pl.BlockSpec(memory_space=pltpu.VMEM)
HBM = pl.BlockSpec(memory_space=pltpu.HBM)
ANY = pl.BlockSpec(memory_space=pl.ANY)


def exchange(pieces, count, wrap=True):
    onward, near, far = pieces
    stop = count if wrap else count - STRIPS
    got_onward = lax.ppermute(
        onward, "bay", [(i, (i + STRIPS) % count) for i in range(stop)]
    )
    got_near = lax.ppermute(near, "bay", [(i, i ^ 1) for i in range(count)])
    got_far = lax.ppermute(far, "bay", [(i, i ^ 2) for i in range(count)])
    return got_onward, got_near, got_far


def fetch(source, outs, spans, sems):
    copies = []
    for index, (out, (rows, columns)) in enumerate(zip(outs, spans)):
        copies.append(pltpu.make_async_copy(source.at[0, rows, columns], out, sems.at[index]))
        copies[-1].start()
    return copies


def cut_body(spans, source, *rest):
    *outs, sems = rest
    for copy in fetch(source, outs, spans, sems):
        copy.wait()


def load_body(spans, trace_map, source, operator, table, *rest):
    *outs, select, weights, loads, order, sems = rest
    fetch_order = pltpu.make_async_copy(trace_map, order, sems.at[len(spans) + 2])
    fetch_order.start()
    copies = fetch(source, outs, spans, sems)
    for index, (whole, out) in enumerate(((operator, weights), (table, loads))):
        copies.append(pltpu.make_async_copy(whole.at[0], out, sems.at[len(spans) + index]))
        copies[-1].start()
    size = order.shape[1]
    block = min(256, size)
    fetch_order.wait()
    wanted = jnp.where(lax.axis_index("bay") >= STRIPS, order[...], -1)
    for top in range(0, size, block):
        rows = top + lax.broadcasted_iota(jnp.int32, (block, size), 0)
        select[top : top + block, :] = (wanted == rows).astype(jnp.bfloat16)
    for copy in copies:
        copy.wait()


def shape_of(span):
    return jax.ShapeDtypeStruct(tuple(part.stop - part.start for part in span), jnp.bfloat16)


def in_hbm(*arrays):
    return [pltpu.with_memory_space_constraint(array, pltpu.HBM) for array in arrays]


def cut(traces, spans):
    return pl.pallas_call(
        functools.partial(cut_body, spans),
        out_shape=tuple(shape_of(span) for span in spans),
        in_specs=[HBM],
        out_specs=(VMEM,) * len(spans),
        scratch_shapes=[pltpu.SemaphoreType.DMA((len(spans),))],
        name="cut",
        compiler_params=pltpu.CompilerParams(vmem_limit_bytes=LIMIT),
    )(*in_hbm(traces))


def load(order, traces, spans, operator, loads):
    shapes = [shape_of(span) for span in spans]
    shapes.append(jax.ShapeDtypeStruct((order.shape[1],) * 2, jnp.bfloat16))
    shapes.extend(jax.ShapeDtypeStruct(whole.shape[1:], jnp.bfloat16) for whole in (operator, loads))
    return pl.pallas_call(
        functools.partial(load_body, spans),
        out_shape=tuple(shapes),
        in_specs=[HBM] * 4,
        out_specs=(VMEM,) * len(shapes),
        scratch_shapes=[
            pltpu.VMEM(order.shape, order.dtype),
            pltpu.SemaphoreType.DMA((len(spans) + 3,)),
        ],
        name="load",
        compiler_params=pltpu.CompilerParams(vmem_limit_bytes=LIMIT),
    )(*in_hbm(order, traces, operator, loads))


def permuted(onward, select):
    return jnp.dot(onward[...], select[...], preferred_element_type=jnp.float32).astype(
        jnp.bfloat16
    )


def amplitudes(tick, chunk, size, seeds, patches, table):
    own = slice(chunk * size, (chunk + 1) * size)
    amplitude = ((seeds[:, own] * 7 + 13 * tick) % 97 - 48).astype(jnp.float32) / 32.0
    rows = lax.broadcasted_iota(jnp.int32, (table.shape[0], size), 0)
    return jnp.where(rows == patches[:, own], amplitude, 0.0).astype(jnp.bfloat16)


def lateral(loaded, near, far, weights, table, low, high):
    split = weights.shape[0] - far.shape[1]
    start = split - near.shape[1]
    total = jnp.dot(near[...], weights[start:split, low:high], preferred_element_type=jnp.float32)
    total += jnp.dot(far[...], weights[split:, low:high], preferred_element_type=jnp.float32)
    total += lax.dot_general(
        loaded, table[:, low:high], (((0,), (0,)), ((), ())), preferred_element_type=jnp.float32
    )
    return total


def block(mapped, loaded, near, far, weights, table, low, high):
    total = lateral(loaded, near, far, weights, table, low, high)
    total += jnp.dot(
        mapped, weights[: mapped.shape[1], low:high], preferred_element_type=jnp.float32
    )
    return total.astype(jnp.bfloat16)


def step_body(tick, chunk, onward, near, far, select, seeds, patches, table, weights, *outs):
    mapped = permuted(onward, select)
    loaded = amplitudes(tick, chunk, onward.shape[0], seeds, patches, table)
    start = 0
    for out in outs:
        for low in range(0, out.shape[1], COLS):
            out[:, low : low + COLS] = block(
                mapped, loaded, near, far, weights, table, start + low, start + low + COLS
            )
        start += out.shape[1]


def late_body(tick, chunk, parts, onward, near, far, seeds, patches, table, weights, *refs):
    uppers, outs = refs[:parts], refs[parts:]
    loaded = amplitudes(tick, chunk, onward.shape[0], seeds, patches, table)
    low, start = 0, 0
    ends = []
    for out in outs:
        start += out.shape[1]
        ends.append(start)
    for upper in uppers:
        high = low + upper.shape[1]
        total = lateral(loaded, near, far, weights, table, low, high)
        total += jnp.dot(onward[...], upper[...], preferred_element_type=jnp.float32)
        for out, end in zip(outs, ends):
            begin = end - out.shape[1]
            if begin <= low < end:
                out[:, low - begin : high - begin] = total.astype(jnp.bfloat16)
        low = high


def late_step(tick, chunk, got, common, weights, uppers):
    return pl.pallas_call(
        functools.partial(late_body, tick, chunk, len(uppers)),
        out_shape=tuple(jax.ShapeDtypeStruct(piece.shape, jnp.bfloat16) for piece in got),
        in_specs=[VMEM] * (len(uppers) + 7),
        out_specs=(VMEM,) * 3,
        compiler_params=pltpu.CompilerParams(vmem_limit_bytes=LIMIT),
        cost_estimate=cost(got[0].shape[0], weights),
    )(*got, *common[1:], weights, *uppers)


def cost(rows, weights):
    return pl.CostEstimate(
        flops=2 * rows * weights.shape[0] * weights.shape[1],
        transcendentals=0,
        bytes_accessed=weights.size * 2,
    )


def step(tick, chunk, got, common, weights):
    return pl.pallas_call(
        functools.partial(step_body, tick, chunk),
        out_shape=tuple(jax.ShapeDtypeStruct(piece.shape, jnp.bfloat16) for piece in got),
        in_specs=[VMEM] * 8,
        out_specs=(VMEM,) * 3,
        compiler_params=pltpu.CompilerParams(vmem_limit_bytes=LIMIT),
        cost_estimate=cost(got[0].shape[0], weights),
    )(*got, *common, weights)


def column_body(low, select, weights, out):
    out[...] = jnp.dot(
        select[...],
        weights[: select.shape[1], low : low + out.shape[1]],
        preferred_element_type=jnp.float32,
    ).astype(jnp.bfloat16)


def columns_of(low, width, select, weights):
    size = select.shape[0]
    return pl.pallas_call(
        functools.partial(column_body, low),
        out_shape=jax.ShapeDtypeStruct((size, width), jnp.bfloat16),
        in_specs=[VMEM] * 2,
        out_specs=VMEM,
        name="columns",
        compiler_params=pltpu.CompilerParams(vmem_limit_bytes=LIMIT),
        cost_estimate=pl.CostEstimate(
            flops=2 * size * size * width, transcendentals=0, bytes_accessed=size * size * 2
        ),
    )(select, weights)


def side_body(tick, chunk, near, far, seeds, patches, table, weights, out):
    loaded = amplitudes(tick, chunk, near.shape[0], seeds, patches, table)
    for low in range(0, out.shape[1], COLS):
        out[:, low : low + COLS] = lateral(loaded, near, far, weights, table, low, low + COLS)


def side(tick, chunk, got, common, weights):
    return pl.pallas_call(
        functools.partial(side_body, tick, chunk),
        out_shape=jax.ShapeDtypeStruct((got[0].shape[0], weights.shape[1]), jnp.float32),
        in_specs=[VMEM] * 6,
        out_specs=VMEM,
        name="side",
        compiler_params=pltpu.CompilerParams(vmem_limit_bytes=LIMIT),
        cost_estimate=cost(got[0].shape[0] // 2, weights),
    )(*got[1:], *common[1:], weights)


def last_body(chunk, parts, onward, beside, *refs):
    uppers = refs[:parts]
    out, buffer, sems = refs[-3:]
    rows = buffer.shape[0]
    copies = []
    low = 0
    for index, upper in enumerate(uppers):
        high = low + upper.shape[1]
        total = beside[:, low:high] + jnp.dot(
            onward[...], upper[...], preferred_element_type=jnp.float32
        )
        buffer[:, low:high] = total.astype(jnp.bfloat16)
        copies.append(
            pltpu.make_async_copy(
                buffer.at[:, low:high],
                out.at[0, chunk * rows : (chunk + 1) * rows, low:high],
                sems.at[index],
            )
        )
        copies[-1].start()
        low = high
    for copy in copies:
        copy.wait()


def last_step(tick, chunk, got, common, weights, uppers, previous):
    rows, width = got[0].shape[0], weights.shape[1]
    extra = [] if previous is None else [previous]
    beside = side(tick, chunk, got, common, weights)
    return pl.pallas_call(
        functools.partial(last_body, chunk, len(uppers)),
        out_shape=jax.ShapeDtypeStruct((1, rows * CHUNKS, width), jnp.bfloat16),
        in_specs=[VMEM] * (len(uppers) + 2) + [ANY] * len(extra),
        out_specs=ANY,
        scratch_shapes=[
            pltpu.VMEM((rows, width), jnp.bfloat16),
            pltpu.SemaphoreType.DMA((len(uppers),)),
        ],
        input_output_aliases={len(uppers) + 2: 0} if extra else {},
        name="last",
        compiler_params=pltpu.CompilerParams(vmem_limit_bytes=LIMIT),
        cost_estimate=cost(rows // 2, weights),
    )(got[0], beside, *uppers, *extra)


def on_device(traces, operator, loads, seeds, patches, trace_map):
    count = lax.axis_size("bay")
    _, rows, width = traces.shape
    onward = trace_map.shape[1]
    near = onward + (width - onward) // 2
    size = rows // CHUNKS
    columns = (slice(0, onward), slice(onward, near), slice(near, width))
    spans = [
        [(slice(c * size, (c + 1) * size), piece) for piece in columns] for c in range(CHUNKS)
    ]
    flat = [span for part in spans for span in part]

    pieces = cut(traces, flat[:EARLY])
    *others, select, weights, table = load(trace_map, traces, flat[EARLY:], operator, loads)
    pieces = [*pieces, *others]
    got = []
    for c in range(CHUNKS):
        got.append(exchange(pieces[3 * c : 3 * c + 3], count))

    common = (select, seeds[None], patches, table)
    uppers = []
    out = None
    for tick in range(TICKS):
        for c in range(CHUNKS):
            if tick == TICKS - 1:
                out = last_step(tick, c, got[c], common, weights, uppers, out)
            else:
                if len(uppers) == PARTS:
                    pieces = late_step(tick, c, got[c], common, weights, uppers)
                else:
                    pieces = step(tick, c, got[c], common, weights)
                if SPARE <= CHUNKS * tick + c < SPARE + PARTS:
                    part = width // PARTS
                    uppers.append(columns_of(len(uppers) * part, part, select, weights))
                got[c] = exchange(pieces, count, (tick, c) != (TICKS - 2, CHUNKS - 1))
    return out


def solution(mesh):
    placed = (
        P("bay", "groups", None),
        P("bay", None, None),
        P("bay", None, None),
        P("groups"),
        P("bay", "groups"),
        P("bay", None),
    )
    return jax.shard_map(
        on_device, mesh=mesh, in_specs=placed, out_specs=P("bay", "groups", None), check_vma=False
    )
```

```python
import functools

import jax
import jax.numpy as jnp
from jax import lax
from jax.experimental import pallas as pl
from jax.experimental.pallas import tpu as pltpu
from jax.sharding import PartitionSpec as P


TICKS = 6
STRIPS = 4
CHUNKS = 2
COLS = 512
EARLY = 4
PARTS = 8
SPARE = 0
LIMIT = 16 << 20


VMEM = pl.BlockSpec(memory_space=pltpu.VMEM)
HBM = pl.BlockSpec(memory_space=pltpu.HBM)
ANY = pl.BlockSpec(memory_space=pl.ANY)


def exchange(pieces, count, wrap=True):
    onward, near, far = pieces
    stop = count if wrap else count - STRIPS
    got_onward = lax.ppermute(
        onward, "bay", [(i, (i + STRIPS) % count) for i in range(stop)]
    )
    got_near = lax.ppermute(near, "bay", [(i, i ^ 1) for i in range(count)])
    got_far = lax.ppermute(far, "bay", [(i, i ^ 2) for i in range(count)])
    return got_onward, got_near, got_far


def fetch(source, outs, spans, sems):
    copies = []
    for index, (out, (rows, columns)) in enumerate(zip(outs, spans)):
        copies.append(pltpu.make_async_copy(source.at[0, rows, columns], out, sems.at[index]))
        copies[-1].start()
    return copies


def cut_body(spans, source, *rest):
    *outs, sems = rest
    for copy in fetch(source, outs, spans, sems):
        copy.wait()


def load_body(spans, trace_map, source, operator, table, *rest):
    *outs, select, weights, loads, order, sems = rest
    fetch_order = pltpu.make_async_copy(trace_map, order, sems.at[len(spans) + 2])
    fetch_order.start()
    copies = fetch(source, outs, spans, sems)
    for index, (whole, out) in enumerate(((operator, weights), (table, loads))):
        copies.append(pltpu.make_async_copy(whole.at[0], out, sems.at[len(spans) + index]))
        copies[-1].start()
    size = order.shape[1]
    block = min(256, size)
    fetch_order.wait()
    wanted = jnp.where(lax.axis_index("bay") >= STRIPS, order[...], -1)
    for top in range(0, size, block):
        rows = top + lax.broadcasted_iota(jnp.int32, (block, size), 0)
        select[top : top + block, :] = (wanted == rows).astype(jnp.bfloat16)
    for copy in copies:
        copy.wait()


def shape_of(span):
    return jax.ShapeDtypeStruct(tuple(part.stop - part.start for part in span), jnp.bfloat16)


def in_hbm(*arrays):
    return [pltpu.with_memory_space_constraint(array, pltpu.HBM) for array in arrays]


def cut(traces, spans):
    return pl.pallas_call(
        functools.partial(cut_body, spans),
        out_shape=tuple(shape_of(span) for span in spans),
        in_specs=[HBM],
        out_specs=(VMEM,) * len(spans),
        scratch_shapes=[pltpu.SemaphoreType.DMA((len(spans),))],
        name="cut",
        compiler_params=pltpu.CompilerParams(vmem_limit_bytes=LIMIT),
    )(*in_hbm(traces))


def load(order, traces, spans, operator, loads):
    shapes = [shape_of(span) for span in spans]
    shapes.append(jax.ShapeDtypeStruct((order.shape[1],) * 2, jnp.bfloat16))
    shapes.extend(jax.ShapeDtypeStruct(whole.shape[1:], jnp.bfloat16) for whole in (operator, loads))
    return pl.pallas_call(
        functools.partial(load_body, spans),
        out_shape=tuple(shapes),
        in_specs=[HBM] * 4,
        out_specs=(VMEM,) * len(shapes),
        scratch_shapes=[
            pltpu.VMEM(order.shape, order.dtype),
            pltpu.SemaphoreType.DMA((len(spans) + 3,)),
        ],
        name="load",
        compiler_params=pltpu.CompilerParams(vmem_limit_bytes=LIMIT),
    )(*in_hbm(order, traces, operator, loads))


def permuted(onward, select):
    return jnp.dot(onward[...], select[...], preferred_element_type=jnp.float32).astype(
        jnp.bfloat16
    )


def amplitudes(tick, chunk, size, seeds, patches, table):
    own = slice(chunk * size, (chunk + 1) * size)
    amplitude = ((seeds[:, own] * 7 + 13 * tick) % 97 - 48).astype(jnp.float32) / 32.0
    rows = lax.broadcasted_iota(jnp.int32, (table.shape[0], size), 0)
    return jnp.where(rows == patches[:, own], amplitude, 0.0).astype(jnp.bfloat16)


def lateral(loaded, near, far, weights, table, low, high):
    split = weights.shape[0] - far.shape[1]
    start = split - near.shape[1]
    total = jnp.dot(near[...], weights[start:split, low:high], preferred_element_type=jnp.float32)
    total += jnp.dot(far[...], weights[split:, low:high], preferred_element_type=jnp.float32)
    total += lax.dot_general(
        loaded, table[:, low:high], (((0,), (0,)), ((), ())), preferred_element_type=jnp.float32
    )
    return total


def block(mapped, loaded, near, far, weights, table, low, high):
    total = lateral(loaded, near, far, weights, table, low, high)
    total += jnp.dot(
        mapped, weights[: mapped.shape[1], low:high], preferred_element_type=jnp.float32
    )
    return total.astype(jnp.bfloat16)


def step_body(tick, chunk, onward, near, far, select, seeds, patches, table, weights, *outs):
    mapped = permuted(onward, select)
    loaded = amplitudes(tick, chunk, onward.shape[0], seeds, patches, table)
    start = 0
    for out in outs:
        for low in range(0, out.shape[1], COLS):
            out[:, low : low + COLS] = block(
                mapped, loaded, near, far, weights, table, start + low, start + low + COLS
            )
        start += out.shape[1]


def late_body(tick, chunk, parts, onward, near, far, seeds, patches, table, weights, *refs):
    uppers, outs = refs[:parts], refs[parts:]
    loaded = amplitudes(tick, chunk, onward.shape[0], seeds, patches, table)
    low, start = 0, 0
    ends = []
    for out in outs:
        start += out.shape[1]
        ends.append(start)
    for upper in uppers:
        high = low + upper.shape[1]
        total = lateral(loaded, near, far, weights, table, low, high)
        total += jnp.dot(onward[...], upper[...], preferred_element_type=jnp.float32)
        for out, end in zip(outs, ends):
            begin = end - out.shape[1]
            if begin <= low < end:
                out[:, low - begin : high - begin] = total.astype(jnp.bfloat16)
        low = high


def late_step(tick, chunk, got, common, weights, uppers):
    return pl.pallas_call(
        functools.partial(late_body, tick, chunk, len(uppers)),
        out_shape=tuple(jax.ShapeDtypeStruct(piece.shape, jnp.bfloat16) for piece in got),
        in_specs=[VMEM] * (len(uppers) + 7),
        out_specs=(VMEM,) * 3,
        compiler_params=pltpu.CompilerParams(vmem_limit_bytes=LIMIT),
        cost_estimate=cost(got[0].shape[0], weights),
    )(*got, *common[1:], weights, *uppers)


def cost(rows, weights):
    return pl.CostEstimate(
        flops=2 * rows * weights.shape[0] * weights.shape[1],
        transcendentals=0,
        bytes_accessed=weights.size * 2,
    )


def step(tick, chunk, got, common, weights):
    return pl.pallas_call(
        functools.partial(step_body, tick, chunk),
        out_shape=tuple(jax.ShapeDtypeStruct(piece.shape, jnp.bfloat16) for piece in got),
        in_specs=[VMEM] * 8,
        out_specs=(VMEM,) * 3,
        compiler_params=pltpu.CompilerParams(vmem_limit_bytes=LIMIT),
        cost_estimate=cost(got[0].shape[0], weights),
    )(*got, *common, weights)


def column_body(low, select, weights, out):
    out[...] = jnp.dot(
        select[...],
        weights[: select.shape[1], low : low + out.shape[1]],
        preferred_element_type=jnp.float32,
    ).astype(jnp.bfloat16)


def columns_of(low, width, select, weights):
    size = select.shape[0]
    return pl.pallas_call(
        functools.partial(column_body, low),
        out_shape=jax.ShapeDtypeStruct((size, width), jnp.bfloat16),
        in_specs=[VMEM] * 2,
        out_specs=VMEM,
        name="columns",
        compiler_params=pltpu.CompilerParams(vmem_limit_bytes=LIMIT),
        cost_estimate=pl.CostEstimate(
            flops=2 * size * size * width, transcendentals=0, bytes_accessed=size * size * 2
        ),
    )(select, weights)


def side_body(tick, chunk, start, near, seeds, patches, table, weights, out):
    loaded = amplitudes(tick, chunk, near.shape[0], seeds, patches, table)
    for low in range(0, out.shape[1], COLS):
        high = low + COLS
        total = jnp.dot(
            near[...],
            weights[start : start + near.shape[1], low:high],
            preferred_element_type=jnp.float32,
        )
        out[:, low:high] = total + lax.dot_general(
            loaded, table[:, low:high], (((0,), (0,)), ((), ())), preferred_element_type=jnp.float32
        )


def side(tick, chunk, got, common, weights):
    return pl.pallas_call(
        functools.partial(side_body, tick, chunk, got[0].shape[1]),
        out_shape=jax.ShapeDtypeStruct((got[0].shape[0], weights.shape[1]), jnp.float32),
        in_specs=[VMEM] * 5,
        out_specs=VMEM,
        name="side",
        compiler_params=pltpu.CompilerParams(vmem_limit_bytes=LIMIT),
        cost_estimate=cost(got[0].shape[0] // 2, weights),
    )(got[1], *common[1:], weights)


def last_body(chunk, parts, onward, far, beside, weights, *refs):
    uppers = refs[:parts]
    out, buffer, sems = refs[-3:]
    rows = buffer.shape[0]
    copies = []
    low = 0
    for index, upper in enumerate(uppers):
        high = low + upper.shape[1]
        total = beside[:, low:high] + jnp.dot(
            onward[...], upper[...], preferred_element_type=jnp.float32
        )
        total += jnp.dot(
            far[...], weights[weights.shape[0] - far.shape[1] :, low:high], preferred_element_type=jnp.float32
        )
        buffer[:, low:high] = total.astype(jnp.bfloat16)
        copies.append(
            pltpu.make_async_copy(
                buffer.at[:, low:high],
                out.at[0, chunk * rows : (chunk + 1) * rows, low:high],
                sems.at[index],
            )
        )
        copies[-1].start()
        low = high
    for copy in copies:
        copy.wait()


def last_step(tick, chunk, got, common, weights, uppers, previous):
    rows, width = got[0].shape[0], weights.shape[1]
    extra = [] if previous is None else [previous]
    beside = side(tick, chunk, got, common, weights)
    return pl.pallas_call(
        functools.partial(last_body, chunk, len(uppers)),
        out_shape=jax.ShapeDtypeStruct((1, rows * CHUNKS, width), jnp.bfloat16),
        in_specs=[VMEM] * (len(uppers) + 4) + [ANY] * len(extra),
        out_specs=ANY,
        scratch_shapes=[
            pltpu.VMEM((rows, width), jnp.bfloat16),
            pltpu.SemaphoreType.DMA((len(uppers),)),
        ],
        input_output_aliases={len(uppers) + 4: 0} if extra else {},
        name="last",
        compiler_params=pltpu.CompilerParams(vmem_limit_bytes=LIMIT),
        cost_estimate=cost(rows // 2, weights),
    )(got[0], got[2], beside, weights, *uppers, *extra)


def on_device(traces, operator, loads, seeds, patches, trace_map):
    count = lax.axis_size("bay")
    _, rows, width = traces.shape
    onward = trace_map.shape[1]
    near = onward + (width - onward) // 2
    size = rows // CHUNKS
    columns = (slice(0, onward), slice(onward, near), slice(near, width))
    spans = [
        [(slice(c * size, (c + 1) * size), piece) for piece in columns] for c in range(CHUNKS)
    ]
    flat = [span for part in spans for span in part]

    pieces = cut(traces, flat[:EARLY])
    *others, select, weights, table = load(trace_map, traces, flat[EARLY:], operator, loads)
    pieces = [*pieces, *others]
    got = []
    for c in range(CHUNKS):
        got.append(exchange(pieces[3 * c : 3 * c + 3], count))

    common = (select, seeds[None], patches, table)
    uppers = []
    out = None
    for tick in range(TICKS):
        for c in range(CHUNKS):
            if tick == TICKS - 1:
                out = last_step(tick, c, got[c], common, weights, uppers, out)
            else:
                if len(uppers) == PARTS:
                    pieces = late_step(tick, c, got[c], common, weights, uppers)
                else:
                    pieces = step(tick, c, got[c], common, weights)
                if SPARE <= CHUNKS * tick + c < SPARE + PARTS:
                    part = width // PARTS
                    uppers.append(columns_of(len(uppers) * part, part, select, weights))
                got[c] = exchange(pieces, count, (tick, c) != (TICKS - 2, CHUNKS - 1))
    return out


def solution(mesh):
    placed = (
        P("bay", "groups", None),
        P("bay", None, None),
        P("bay", None, None),
        P("groups"),
        P("bay", "groups"),
        P("bay", None),
    )
    return jax.shard_map(
        on_device, mesh=mesh, in_specs=placed, out_specs=P("bay", "groups", None), check_vma=False
    )
```
